32 devices in a mesh: dp: 8 (over z, x), mp: 4 (over y, core).
Axes of the slice: x: 2, y: 2, z: 4, core: 2. Of those that a mesh axis runs over, the one named last changes fastest.
Arguments:
- tokens: bfloat16 [2048, 2048], P('dp'), may hold values from -6 to 6
- targets: bfloat16 [2048, 2048], P('dp'), may hold values from -6 to 6
- loss_weights: float32 [2048], P('dp'), may hold values from 0.4 to 14, as said below
- segments: int32 [8, 256], P('dp'), may hold values from 0 to 3, never falling along the last dimension, each value on 1 to 128 neighbouring positions
- probe_model: int32 [8, 2048], P('dp'), may hold values from 0 to 1
- probe_heads: int32 [8, 2, 2048], P('dp', None, 'mp'), may hold values from 0 to 1
- norm_gain: float32 [2048], replicated, may hold values from 0.5 to 1.5
- w_query: bfloat16 [2048, 2048], P(None, 'mp'), may hold values from -0.125 to 0.125
- w_key: bfloat16 [2048, 2048], P(None, 'mp'), may hold values from -0.125 to 0.125
- w_value: bfloat16 [2048, 2048], P(None, 'mp'), may hold values from -0.125 to 0.125
- w_out: bfloat16 [2048, 2048], P('mp'), may hold values from -0.125 to 0.125
Outputs:
- diag_query: float32 [2048, 2048], P('dp', 'mp')
- diag_key: float32 [2048, 2048], P('dp', 'mp')
- mean_diag: float32 [2], replicated
The draws below stay inside these ranges and needn't reach their ends.
Inputs may be any that keep to these rules, and one draw needn't show every extreme that they name: `segments`: the documents of a sequence are runs of 1 to 128 tokens, numbered upwards from 0. `loss_weights`: positive weights.
All inputs are finite; a program needn't handle non-finite values.
Results may differ from the reference program's by a relative error of at most 0.0099.
Values may be sent and summed in bfloat16 or wider, within the bound.
A program may use at most 128 MiB of HBM per device.

```python
import math
import jax
import jax.numpy as jnp
import numpy as np
from jax import lax

D = 2048
HEAD_DIM = 128
SEQ = 256
DOCS = 4
GROUPS = 8
TOKENS = 2048
FEAT = 2048


def draw_loss_weights(key, part):
    group_index = (jnp.arange(TOKENS, dtype=jnp.int32) // SEQ).astype(jnp.float32)
    rising = 1.0 + 2.0 * group_index / max(GROUPS - 1, 1)
    base_values = jnp.exp(jax.random.uniform(key, (TOKENS,), jnp.float32, jnp.log(0.5), jnp.log(2.0)))
    return (rising * base_values).astype(jnp.float32)


def plant(values, key, least, largest):
    place = [jax.random.randint(jax.random.fold_in(key, axis), (), 0, length) for axis, length in enumerate(values.shape)]
    widest = values.shape.index(max(values.shape))
    next_to = place[:widest] + [(place[widest] + 1) % values.shape[widest]] + place[widest + 1:]
    return values.at[tuple(place)].set(least).at[tuple(next_to)].set(largest)


def with_spikes(array, stream_key, source, target, blocks, factor):
    owner, partner = [(jnp.arange(array.shape[axis_at]) // (array.shape[axis_at] // blocks)).reshape([-1 if axis == axis_at else 1 for axis in range(array.ndim)]) for axis_at in (source, target)]
    chosen = jax.random.permutation(stream_key, blocks)[partner]
    strong = (owner == chosen) | (owner == (partner + blocks // 2) % blocks)
    return jnp.where(strong, factor * array, array)


def block_scale(stream_key, dims, shards, low, top_value):
    level, own = 1.0, jax.random.fold_in(stream_key, 6)
    for dim, blocks in shards:
        steps = jnp.exp(jax.random.uniform(jax.random.fold_in(own, dim), (blocks,), jnp.float32, low / len(shards), top_value / len(shards)))
        level = level * jnp.repeat(steps, dims[dim] // blocks).reshape([-1 if axis == dim else 1 for axis in range(len(dims))])
    return level


def profile(count, total, reach, skew):
    loads = [(1 << 20) // math.isqrt(standing ** skew) + 1 for standing in range(2, count + 1)]
    surplus, given = total - reach - (count - 1), [1] * (count - 1)
    while surplus > 0:
        movable = [i for i in range(count - 1) if given[i] < reach]
        whole, left = sum([loads[i] for i in movable]), surplus
        for i in movable:
            extra = min(reach - given[i], max(1, left * loads[i] // whole), surplus)
            given[i] = given[i] + extra
            surplus = surplus - extra
    return np.array([reach] + given)


def ragged_sizes(rng, amount, total, most, slope):
    if amount == 2:
        one = jax.random.randint(rng, (), max(1, total - most), min(most, total - 1) + 1)
        return jnp.stack([one, total - one])
    sizes = jnp.asarray(profile(amount, total, most, slope), jnp.int32)
    twos = (amount - 1) // 2
    source_of, sink = sizes[1:1 + 2 * twos:2], sizes[2:2 + 2 * twos:2]
    slack = jnp.minimum(source_of - 1, most - sink)
    moved = jax.random.randint(jax.random.fold_in(rng, 1), (twos,), 0, 1 << 20) % (slack + 1)
    sizes = sizes.at[1:1 + 2 * twos:2].set(source_of - moved).at[2:2 + 2 * twos:2].set(sink + moved)
    return sizes[jax.random.permutation(jax.random.fold_in(rng, 2), amount)]


def gaussian(key, dims, spread, most, split=(), kind=jnp.bfloat16):
    gain = block_scale(key, dims, split, -0.22, 0.18) if split else 1.0
    values = jax.random.normal(key, dims, jnp.float32) * spread * gain
    return jnp.minimum(jnp.maximum(values, -most), most).astype(kind)


def heavy_noise(key, shape, scale, limit, pieces, heavy, kind=jnp.bfloat16):
    values = scale * jax.random.normal(key, shape, jnp.float32)
    if pieces:
        values = values * block_scale(key, shape, pieces, -0.22, 0.18)
    return jnp.clip(with_spikes(values, jax.random.fold_in(key, 3), *heavy), -limit, limit).astype(kind)


def setup_inputs(seed: int = 0) -> dict:
    seeds = jax.random.split(jax.random.key(seed), 12)
    tokens = heavy_noise(seeds[0], (TOKENS, D), 1.0, 6.0, ((0, 8),), (0, 1, 8, 2.0))
    targets = heavy_noise(seeds[1], (TOKENS, D), 1.0, 6.0, ((0, 8),), (0, 1, 8, 2.0))
    loss_weights = draw_loss_weights(jax.random.fold_in(seeds[11], 71), 0)
    segments = jax.vmap(lambda own: jnp.searchsorted(jnp.cumsum(ragged_sizes(own, DOCS, SEQ, SEQ // 2, 0)), jnp.arange(SEQ), side="right"))(jax.random.split(seeds[3], GROUPS)).reshape((GROUPS, SEQ)).astype(jnp.int32)
    probe_model = plant(jax.random.randint(seeds[4], (GROUPS, D), 0, 2), jax.random.fold_in(seeds[4], 1), 0, 1).astype(jnp.int32)
    probe_heads = plant(jax.random.randint(seeds[5], (GROUPS, 2, FEAT), 0, 2), jax.random.fold_in(seeds[5], 1), 0, 1).astype(jnp.int32)
    norm_gain = jnp.clip(1.0 + 0.1 * jax.random.normal(seeds[6], (D,), jnp.float32), 0.5, 1.5)
    w_query = gaussian(seeds[7], (D, FEAT), D ** -0.5, 0.125, ((1, 4),))
    w_key = gaussian(seeds[8], (D, FEAT), D ** -0.5, 0.125, ((1, 4),))
    w_value = gaussian(seeds[9], (D, FEAT), D ** -0.5, 0.125, ((1, 4),))
    w_out = gaussian(seeds[10], (FEAT, D), FEAT ** -0.5, 0.125, ((0, 4),))
    return dict(tokens=tokens, targets=targets, loss_weights=loss_weights, segments=segments, probe_model=probe_model, probe_heads=probe_heads, norm_gain=norm_gain, w_query=w_query, w_key=w_key, w_value=w_value, w_out=w_out)


exact_mode = lax.Precision.HIGHEST
norm_epsilon = 1e-06

def sign_pattern(row_index, col_index):
    mixed_index = (row_index[:, None] * 1103 + col_index[None, :] * 2713 + 7) % 32749
    mixed_index = mixed_index * mixed_index % 32749
    return 1.0 - 2.0 * (mixed_index // 5 % 2).astype(jnp.float32)

def rope_tables(length):
    position = jnp.arange(length, dtype=jnp.int32).astype(jnp.float32)
    exponent = jnp.arange(0, HEAD_DIM, 2, dtype=jnp.int32).astype(jnp.float32) / HEAD_DIM
    frequency = 10000.0 ** (-exponent)
    angles = position[:, None] * frequency[None, :]
    return (jnp.cos(angles)[:, None, :], jnp.sin(angles)[:, None, :])

def rotate(packed, cosine, sine_table):
    half_dim = packed.shape[-1] // 2
    front_half = packed[..., :half_dim]
    back_half = packed[..., half_dim:]
    return jnp.concatenate([front_half * cosine - back_half * sine_table, back_half * cosine + front_half * sine_table], axis=-1)

def attend(query, keys, values, doc_ids):
    length = query.shape[0]
    head_count = query.shape[1] // HEAD_DIM
    cosine, sine_table = rope_tables(length)
    rotated_query = rotate(query.reshape(length, head_count, HEAD_DIM), cosine, sine_table)
    rotated_keys = rotate(keys.reshape(length, head_count, HEAD_DIM), cosine, sine_table)
    scores = jnp.einsum('qhd,khd->hqk', rotated_query, rotated_keys, precision=exact_mode) * HEAD_DIM ** (-0.5)
    position = jnp.arange(length, dtype=jnp.int32)
    allowed = (position[:, None] >= position[None, :]) & (doc_ids[:, None] == doc_ids[None, :])
    raised = jnp.where(allowed[None], jnp.exp(scores), 0.0)
    attention_weights = raised / lax.optimization_barrier(jnp.sum(raised, axis=-1, keepdims=True))
    mixed_values = jnp.einsum('hqk,khd->qhd', attention_weights, values.reshape(length, head_count, HEAD_DIM), precision=exact_mode)
    return mixed_values.reshape(length, head_count * HEAD_DIM)

def tangent_of(query, keys, values, doc_ids, tangents):

    def forward(query_in, keys_in, values_in):
        return attend(query_in, keys_in, values_in, doc_ids)
    result, pullback = jax.vjp(forward, query, keys, values)

    def pulled(cotangent):
        return pullback(cotangent)
    unused, pushforward = jax.vjp(pulled, jnp.zeros_like(result))
    return (result, pushforward((tangents[0], tangents[1], jnp.zeros_like(values)))[0])

def second_order(query, keys, values, doc_ids, back_grad, tangents, back_tangent):

    def inner(query_in, keys_in):

        def paired(query_at, keys_at):
            return jnp.sum(attend(query_at, keys_at, values, doc_ids) * back_grad)
        gradients = jax.grad(paired, argnums=(0, 1))(query_in, keys_in)
        summed = jnp.sum(gradients[0] * tangents[0]) + jnp.sum(gradients[1] * tangents[1])
        return summed + jnp.sum(attend(query_in, keys_in, values, doc_ids) * back_tangent)
    return jax.grad(inner, argnums=(0, 1))(query, keys)

def bf_dot(left, right):
    return jnp.dot(left, right, preferred_element_type=jnp.float32)

def reference(tokens, targets, loss_weights, segments, probe_model, probe_heads, norm_gain, w_query, w_key, w_value, w_out):
    pattern = sign_pattern(jnp.arange(D, dtype=jnp.int32), jnp.arange(FEAT, dtype=jnp.int32))

    def group_step(carry, inputs):
        group_tokens, group_targets, group_weights, doc_ids, model_bits, head_bits = inputs
        model_sign = 2.0 * model_bits.astype(jnp.float32) - 1.0
        head_sign = 2.0 * head_bits.astype(jnp.float32) - 1.0
        probe_query = (model_sign[:, None] * head_sign[0][None, :] * pattern).astype(jnp.bfloat16)
        probe_key = (model_sign[:, None] * head_sign[1][None, :] * pattern).astype(jnp.bfloat16)
        token_float = group_tokens.astype(jnp.float32)
        inverse_rms = lax.rsqrt(lax.optimization_barrier(jnp.mean(token_float * token_float, axis=1, keepdims=True)) + norm_epsilon)
        normed = (token_float * inverse_rms * norm_gain).astype(jnp.bfloat16)
        query = bf_dot(normed, w_query)
        keys = bf_dot(normed, w_key)
        values = bf_dot(normed, w_value)
        d_query = bf_dot(normed, probe_query)
        d_keys = bf_dot(normed, probe_key)
        attended_full, d_attended_full = tangent_of(query, keys, values, doc_ids, (d_query, d_keys))
        attended = attended_full.astype(jnp.bfloat16)
        d_attended = d_attended_full.astype(jnp.bfloat16)
        weight_rows = group_weights / SEQ
        output = token_float + bf_dot(attended, w_out)
        residual = ((output - group_targets.astype(jnp.float32)) * weight_rows[:, None]).astype(jnp.bfloat16)
        d_output = bf_dot(d_attended, w_out)
        d_residual = (d_output * weight_rows[:, None]).astype(jnp.bfloat16)
        back_grad = bf_dot(residual, w_out.T)
        back_tangent = bf_dot(d_residual, w_out.T)
        h_query, h_keys = second_order(query, keys, values, doc_ids, back_grad, (d_query, d_keys), back_tangent)
        est_query = probe_query.astype(jnp.float32) * bf_dot(normed.T, h_query.astype(jnp.bfloat16))
        est_key = probe_key.astype(jnp.float32) * bf_dot(normed.T, h_keys.astype(jnp.bfloat16))
        return ((carry[0] + est_query, carry[1] + est_key), None)
    zero_feat = jnp.zeros((D, FEAT), jnp.float32)
    inputs = (tokens.reshape(GROUPS, SEQ, D), targets.reshape(GROUPS, SEQ, D), loss_weights.reshape(GROUPS, SEQ), segments, probe_model, probe_heads)
    sums, unused = lax.scan(group_step, (zero_feat, zero_feat), inputs)
    diag_query = sums[0] / GROUPS
    diag_key = sums[1] / GROUPS
    mean_diag = jnp.stack([jnp.sum(diag_query), jnp.sum(diag_key)]) / (D * FEAT)
    return (diag_query, diag_key, mean_diag)
```

```python
import functools

import jax
import jax.numpy as jnp
from jax import lax
from jax.experimental import pallas as pl
from jax.experimental.pallas import tpu as pltpu
from jax.sharding import PartitionSpec as P

HEAD_DIM = 128
PRIME = 32749
CHUNKS = 2
EXACT = lax.Precision.HIGHEST
F32 = jnp.float32
BF16 = jnp.bfloat16
MESH = pl.DeviceIdType.MESH

NN = (((1,), (0,)), ((), ()))
NT = (((1,), (1,)), ((), ()))
TN = (((0,), (0,)), ((), ()))


def dot(left, right, dims=NN, precision=None):
    return lax.dot_general(left, right, dims, precision=precision, preferred_element_type=F32)


def low(left, right, dims=NN):
    return dot(left.astype(BF16), right.astype(BF16), dims)


def residue(whole):
    value = whole.astype(F32)
    left = value - jnp.floor(value * (1.0 / PRIME)) * PRIME
    left = jnp.where(left < 0, left + PRIME, left)
    left = jnp.where(left >= PRIME, left - PRIME, left)
    return left.astype(jnp.int32)


def pattern_block(row_part, col_part):
    mixed = row_part + col_part
    mixed = jnp.where(mixed >= PRIME, mixed - PRIME, mixed)
    square = mixed * mixed
    times = (square.astype(F32) * (1.0 / PRIME)).astype(jnp.int32)
    left = square - times * PRIME
    left = jnp.where(left < 0, left + PRIME, left)
    left = jnp.where(left >= PRIME, left - PRIME, left)
    odd = jnp.bitwise_and(jnp.right_shift(left * 52429, 18), 1)
    return jnp.where(odd == 1, -1.0, 1.0).astype(BF16)


def kernel(
    groups,
    parts,
    entries,
    tokens,
    targets,
    row_weights,
    seg_col,
    seg_row,
    model_sign,
    head_sign,
    gain,
    cosine,
    sine,
    wq_hbm,
    wk_hbm,
    wv_hbm,
    wo_hbm,
    diag_query,
    diag_key,
    mean_out,
    wq,
    wk,
    wv,
    wo,
    normed,
    signed,
    turned,
    turned_all,
    pattern,
    query,
    keys,
    values,
    product,
    soft,
    d_soft,
    attended,
    out_send,
    own_part,
    pair_recv,
    chip_send,
    chip_recv,
    residual,
    hk_sum,
    gathered,
    stat_send,
    stat_recv,
    stat_all,
    w_sem,
    turn_send,
    turn_recv,
    pair_ssem,
    pair_rsem,
    chip_ssem,
    chip_rsem,
    res_ssem,
    res_rsem,
    line_ssem,
    line_rsem,
    x_ssem,
    stat_ssem,
    stat_rsem,
    all_ssem,
    all_rsem,
):
    seq, width = tokens.shape
    feat = wq.shape[1]
    heads = feat // HEAD_DIM
    block = width // groups
    rows = seq // CHUNKS
    dp = lax.axis_index("dp")
    mp = lax.axis_index("mp")
    kind = lax.rem(mp, 2)
    other = 1 - kind
    pair = mp + 1 - 2 * kind
    chip = lax.rem(mp + 2, parts)
    inner = lax.rem(dp, 2)
    outer = dp // 2
    lines = groups // 2
    x_peer = dp + 1 - 2 * inner

    loads = []
    for n, (source, target) in enumerate(((wq_hbm, wq), (wk_hbm, wk), (wv_hbm, wv), (wo_hbm, wo))):
        load = pltpu.make_async_copy(source, target, w_sem.at[n])
        load.start()
        loads.append(load)

    barrier = pltpu.get_barrier_semaphore()
    for step in range(1, groups):
        pl.semaphore_signal(barrier, inc=1, device_id={"dp": lax.rem(dp + step, groups)}, device_id_type=MESH)
    pl.semaphore_signal(barrier, inc=1, device_id={"mp": pair}, device_id_type=MESH)
    pl.semaphore_signal(barrier, inc=1, device_id={"mp": chip}, device_id_type=MESH)

    token_float = tokens[...].astype(F32)
    inverse = lax.rsqrt(jnp.sum(token_float * token_float, axis=1, keepdims=True) / width + 1e-06)
    for start in range(0, width, 256):
        cols = slice(start, start + 256)
        part = (tokens[:, cols].astype(F32) * inverse * gain[:, cols]).astype(BF16)
        normed[:, cols] = part
        part_signed = part.astype(F32) * model_sign[:, cols]
        signed[:, cols] = part_signed.astype(BF16)
        turned[start : start + 256, :] = jnp.transpose(part_signed).astype(BF16)

    pl.semaphore_wait(barrier, groups + 1)

    turns = []
    for step in range(1, groups):
        peer = lax.rem(dp + step, groups)
        turn = pltpu.make_async_remote_copy(
            src_ref=turned.at[pl.ds(pl.multiple_of(peer * block, block), block), :],
            dst_ref=turned_all.at[dp],
            send_sem=turn_send.at[step],
            recv_sem=turn_recv.at[step],
            device_id={"dp": peer},
            device_id_type=MESH,
        )
        turn.start()
        turns.append(turn)

    first_col = mp * feat
    col_part = residue((first_col + lax.broadcasted_iota(jnp.int32, (1, feat), 1)) * 2713)
    total = jnp.zeros((seq, feat), F32)
    for start in range(0, width, 256):
        row_part = residue((start + lax.broadcasted_iota(jnp.int32, (256, 1), 0)) * 1103 + 7)
        signs = pattern_block(row_part, col_part)
        pattern[start : start + 256, :] = signs
        total = total + dot(signed[:, start : start + 256], signs)
    product[...] = total
    loads[0].wait()
    query[...] = dot(normed[...], wq[...])
    loads[1].wait()
    keys[...] = dot(normed[...], wk[...])
    loads[2].wait()
    values[...] = dot(normed[...], wv[...])

    cos = cosine[...]
    sin = sine[...]

    def rotate(array, cos_rows, sin_rows):
        return array * cos_rows + pltpu.roll(array, HEAD_DIM // 2, 1) * sin_rows

    def unrotate(array, cos_rows, sin_rows):
        return array * cos_rows - pltpu.roll(array, HEAD_DIM // 2, 1) * sin_rows

    scale = HEAD_DIM ** (-0.5)
    position_q = lax.broadcasted_iota(jnp.int32, (seq, seq), 0)
    position_k = lax.broadcasted_iota(jnp.int32, (seq, seq), 1)
    allowed = (position_q >= position_k) & (seg_col[...] == seg_row[...])
    for h in range(heads):
        cols = slice(h * HEAD_DIM, (h + 1) * HEAD_DIM)
        q = rotate(query[:, cols], cos, sin)
        k = rotate(keys[:, cols], cos, sin)
        probe = product[:, cols]
        dq = rotate(probe * head_sign[0:1, cols], cos, sin)
        dk = rotate(probe * head_sign[1:2, cols], cos, sin)
        scores = dot(q, k, NT, EXACT) * scale
        d_scores = dot(
            jnp.concatenate([dq, q], axis=1), jnp.concatenate([k, dk], axis=1), NT, EXACT
        ) * scale
        raised = jnp.where(allowed, jnp.exp(scores), 0.0)
        p = raised / jnp.sum(raised, axis=1, keepdims=True)
        d_p = p * (d_scores - jnp.sum(p * d_scores, axis=1, keepdims=True))
        soft[h] = p
        d_soft[h] = d_p
        v = values[:, cols]
        attended[0, :, cols] = low(p, v).astype(BF16)
        attended[1, :, cols] = low(d_p, v).astype(BF16)

    loads[3].wait()

    def pair_copy(c):
        return pltpu.make_async_remote_copy(
            src_ref=out_send.at[pl.ds(c * rows, rows), :],
            dst_ref=pair_recv.at[pl.ds(c * rows, rows), :],
            send_sem=pair_ssem.at[c],
            recv_sem=pair_rsem.at[c],
            device_id={"mp": pair},
            device_id_type=MESH,
        )

    def chip_copy(c):
        return pltpu.make_async_remote_copy(
            src_ref=chip_send.at[pl.ds(c * rows, rows), :],
            dst_ref=chip_recv.at[pl.ds(c * rows, rows), :],
            send_sem=chip_ssem.at[c],
            recv_sem=chip_rsem.at[c],
            device_id={"mp": chip},
            device_id_type=MESH,
        )

    def res_copy(c, which):
        return pltpu.make_async_remote_copy(
            src_ref=residual.at[which, pl.ds(c * rows, rows), :],
            dst_ref=residual.at[which, pl.ds(c * rows, rows), :],
            send_sem=res_ssem.at[c],
            recv_sem=res_rsem.at[c],
            device_id={"mp": pair},
            device_id_type=MESH,
        )

    order = list(range(CHUNKS))[::-1]
    for c in order:
        span = slice(c * rows, (c + 1) * rows)
        out_send[span, :] = dot(attended[other, span, :], wo[...]).astype(BF16)
        pair_copy(c).start()
        own_part[span, :] = dot(attended[kind, span, :], wo[...])
    for c in order:
        span = slice(c * rows, (c + 1) * rows)
        pair_copy(c).wait_recv()
        summed = own_part[span, :] + pair_recv[span, :].astype(F32)
        own_part[span, :] = summed
        chip_send[span, :] = summed.astype(BF16)
        chip_copy(c).start()

    def line_copy(c, slot, target, way):
        return pltpu.make_async_remote_copy(
            src_ref=gathered.at[c, slot],
            dst_ref=gathered.at[c, slot],
            send_sem=line_ssem.at[c, way, slot],
            recv_sem=line_rsem.at[c, slot],
            device_id={"dp": target},
            device_id_type=MESH,
        )

    def x_copy(c, slot):
        return pltpu.make_async_remote_copy(
            src_ref=gathered.at[c, slot],
            dst_ref=gathered.at[c, slot],
            send_sem=x_ssem.at[c, slot],
            recv_sem=line_rsem.at[c, slot],
            device_id={"dp": x_peer},
            device_id_type=MESH,
        )

    def send_own(c):
        @pl.when(outer + 1 < lines)
        def _():
            line_copy(c, dp, dp + 2, 0).start()

        @pl.when(outer >= 1)
        def _():
            line_copy(c, dp, dp - 2, 1).start()

        x_copy(c, dp).start()

    def relay(c, step):
        @pl.when(outer - step >= 0)
        def _():
            slot = dp - 2 * step
            line_copy(c, slot, dp, 0).wait_recv()

            @pl.when(outer + 1 < lines)
            def _():
                line_copy(c, slot, dp + 2, 0).start()

            x_copy(c, slot).start()

        @pl.when(outer + step < lines)
        def _():
            slot = dp + 2 * step
            line_copy(c, slot, dp, 1).wait_recv()

            @pl.when(outer >= 1)
            def _():
                line_copy(c, slot, dp - 2, 1).start()

            x_copy(c, slot).start()

    wanted = jnp.where(kind == 0, 1.0, 0.0)
    sum_q = jnp.zeros((1, HEAD_DIM), F32)
    sum_k = jnp.zeros((1, HEAD_DIM), F32)
    for c in order:
        span = slice(c * rows, (c + 1) * rows)
        reach = (c + 1) * rows
        chip_copy(c).wait_recv()
        whole = own_part[span, :] + chip_recv[span, :].astype(F32)
        shift = tokens[span, :].astype(F32) - targets[span, :].astype(F32)
        residual[kind, span, :] = ((whole + wanted * shift) * row_weights[span, :]).astype(BF16)
        res_copy(c, kind).start()
        back_own = dot(residual[kind, span, :], wo[...], NT)
        res_copy(c, other).wait_recv()
        back_other = dot(residual[other, span, :], wo[...], NT)
        back = jnp.where(kind == 0, back_own, back_other)
        back_tangent = jnp.where(kind == 0, back_other, back_own)
        cos_q = cos[span, :]
        sin_q = sin[span, :]
        cos_k = cos[:reach, :]
        sin_k = sin[:reach, :]
        for h in range(heads):
            cols = slice(h * HEAD_DIM, (h + 1) * HEAD_DIM)
            q = rotate(query[span, cols], cos_q, sin_q)
            k = rotate(keys[:reach, cols], cos_k, sin_k)
            dq = rotate(product[span, cols] * head_sign[0:1, cols], cos_q, sin_q)
            dk = rotate(product[:reach, cols] * head_sign[1:2, cols], cos_k, sin_k)
            v = values[:reach, cols]
            p = soft[h, span, :reach]
            d_p = d_soft[h, span, :reach]
            u = low(back[:, cols], v, NT)
            u_tangent = low(back_tangent[:, cols], v, NT)
            centered = u - jnp.sum(p * u, axis=1, keepdims=True)
            level = jnp.sum(d_p * u + p * u_tangent, axis=1, keepdims=True)
            mixed = (d_p * centered + p * (u_tangent - level)) * scale
            first = p * centered * scale
            both = jnp.concatenate([mixed, first], axis=1)
            hq = unrotate(low(both, jnp.concatenate([k, dk], axis=0)), cos_q, sin_q)
            stacked = jnp.concatenate([mixed, first], axis=0)
            hk = low(stacked, jnp.concatenate([q, dq], axis=0), TN)
            if c == CHUNKS - 1:
                hk_sum[:, cols] = hk
            else:
                hk_sum[:reach, cols] = hk_sum[:reach, cols] + hk
            hk = unrotate(hk_sum[span, cols], cos_q, sin_q)
            hq = (hq.astype(BF16).astype(F32) * head_sign[0:1, cols]).astype(BF16)
            hk = (hk.astype(BF16).astype(F32) * head_sign[1:2, cols]).astype(BF16)
            gathered[c, dp, :, cols] = hq
            gathered[c, dp, :, slice(feat + h * HEAD_DIM, feat + (h + 1) * HEAD_DIM)] = hk
            probe = product[span, cols]
            sum_q = sum_q + jnp.sum(hq.astype(F32) * probe, axis=0, keepdims=True)
            sum_k = sum_k + jnp.sum(hk.astype(F32) * probe, axis=0, keepdims=True)
        send_own(c)
        if c != order[-1]:
            relay(c, 1)

    lane = lax.broadcasted_iota(jnp.int32, (1, HEAD_DIM), 1)
    local = jnp.where(
        lane < HEAD_DIM // 2,
        jnp.sum(sum_q, axis=1, keepdims=True),
        jnp.sum(sum_k, axis=1, keepdims=True),
    )

    def stat_copy(n, peer):
        return pltpu.make_async_remote_copy(
            src_ref=stat_send.at[n],
            dst_ref=stat_recv.at[n],
            send_sem=stat_ssem.at[n],
            recv_sem=stat_rsem.at[n],
            device_id={"mp": peer},
            device_id_type=MESH,
        )

    stat_send[0] = local
    stat_copy(0, pair).start()
    for c in order[:-1]:
        for step in range(2, lines):
            relay(c, step)
    stat_copy(0, pair).wait_recv()
    stat_send[1] = stat_send[0] + stat_recv[0]
    stat_copy(1, chip).start()
    relay(order[-1], 1)
    stat_copy(1, chip).wait_recv()
    stat_all[dp] = stat_send[1] + stat_recv[1]

    def all_copy(step):
        return pltpu.make_async_remote_copy(
            src_ref=stat_all.at[dp],
            dst_ref=stat_all.at[dp],
            send_sem=all_ssem.at[step],
            recv_sem=all_rsem.at[step],
            device_id={"dp": lax.rem(dp + step, groups)},
            device_id_type=MESH,
        )

    for step in range(1, groups):
        all_copy(step).start()
    for step in range(2, lines):
        relay(order[-1], step)

    for turn in turns:
        turn.wait_recv()
    turned_all[dp] = turned[pl.ds(pl.multiple_of(dp * block, block), block), :]
    for c in order:
        for o in range(lines):
            x_copy(c, 2 * o + 1 - inner).wait_recv()

    result = jnp.zeros((block, 2 * feat), F32)
    for g in range(groups):
        for c in range(CHUNKS):
            result = result + dot(turned_all[g, :, c * rows : (c + 1) * rows], gathered[c, g])
    signs = pattern[pl.ds(pl.multiple_of(dp * block, block), block), :].astype(F32) * (1.0 / groups)
    diag_query[...] = result[:, :feat] * signs
    diag_key[...] = result[:, feat:] * signs
    for step in range(1, groups):
        all_copy(step).wait_recv()
    mean_out[...] = jnp.sum(stat_all[...], axis=0) * (1.0 / groups) / entries

    for turn in turns:
        turn.wait_send()
    for c in order:
        pair_copy(c).wait_send()
        chip_copy(c).wait_send()
        res_copy(c, kind).wait_send()
        for step in range(0, lines):
            @pl.when((outer - step >= 0) & (outer + 1 < lines))
            def _():
                line_copy(c, dp - 2 * step, dp + 2, 0).wait_send()

            @pl.when((outer + step < lines) & (outer >= 1))
            def _():
                line_copy(c, dp + 2 * step, dp - 2, 1).wait_send()

        for o in range(lines):
            x_copy(c, 2 * o + inner).wait_send()
    stat_copy(0, pair).wait_send()
    stat_copy(1, chip).wait_send()
    for step in range(1, groups):
        all_copy(step).wait_send()


def local(
    tokens,
    targets,
    loss_weights,
    segments,
    probe_model,
    probe_heads,
    norm_gain,
    w_query,
    w_key,
    w_value,
    w_out,
):
    groups = lax.axis_size("dp")
    parts = lax.axis_size("mp")
    assert parts == 4 and groups % 2 == 0
    seq, width = tokens.shape
    feat = w_query.shape[1]
    heads = feat // HEAD_DIM
    block = width // groups
    rows = seq // CHUNKS
    position = jnp.arange(seq, dtype=jnp.int32).astype(F32)
    exponent = jnp.arange(0, HEAD_DIM, 2, dtype=jnp.int32).astype(F32) / HEAD_DIM
    angles = position[:, None] * (10000.0 ** (-exponent))[None, :]
    cos, sin = jnp.cos(angles), jnp.sin(angles)
    cosine = jnp.concatenate([cos, cos], axis=1)
    sine = jnp.concatenate([-sin, sin], axis=1)
    vmem = pl.BlockSpec(memory_space=pltpu.VMEM)
    anywhere = pl.BlockSpec(memory_space=pl.ANY)
    dma = pltpu.SemaphoreType.DMA
    diag_query, diag_key, means = pl.pallas_call(
        functools.partial(kernel, groups, parts, float(width * feat * parts)),
        out_shape=(
            jax.ShapeDtypeStruct((block, feat), F32),
            jax.ShapeDtypeStruct((block, feat), F32),
            jax.ShapeDtypeStruct((1, HEAD_DIM), F32),
        ),
        in_specs=[vmem] * 10 + [anywhere] * 4,
        out_specs=(vmem, vmem, vmem),
        scratch_shapes=[
            pltpu.VMEM((width, feat), BF16),
            pltpu.VMEM((width, feat), BF16),
            pltpu.VMEM((width, feat), BF16),
            pltpu.VMEM((feat, width), BF16),
            pltpu.VMEM((seq, width), BF16),
            pltpu.VMEM((seq, width), BF16),
            pltpu.VMEM((width, seq), BF16),
            pltpu.VMEM((groups, block, seq), BF16),
            pltpu.VMEM((width, feat), BF16),
            pltpu.VMEM((seq, feat), F32),
            pltpu.VMEM((seq, feat), F32),
            pltpu.VMEM((seq, feat), F32),
            pltpu.VMEM((seq, feat), F32),
            pltpu.VMEM((heads, seq, seq), F32),
            pltpu.VMEM((heads, seq, seq), F32),
            pltpu.VMEM((2, seq, feat), BF16),
            pltpu.VMEM((seq, width), BF16),
            pltpu.VMEM((seq, width), F32),
            pltpu.VMEM((seq, width), BF16),
            pltpu.VMEM((seq, width), BF16),
            pltpu.VMEM((seq, width), BF16),
            pltpu.VMEM((2, seq, width), BF16),
            pltpu.VMEM((seq, feat), F32),
            pltpu.VMEM((CHUNKS, groups, rows, 2 * feat), BF16),
            pltpu.VMEM((2, 1, HEAD_DIM), F32),
            pltpu.VMEM((2, 1, HEAD_DIM), F32),
            pltpu.VMEM((groups, 1, HEAD_DIM), F32),
            dma((4,)),
            dma((groups,)),
            dma((groups,)),
            dma((CHUNKS,)),
            dma((CHUNKS,)),
            dma((CHUNKS,)),
            dma((CHUNKS,)),
            dma((CHUNKS,)),
            dma((CHUNKS,)),
            dma((CHUNKS, 2, groups)),
            dma((CHUNKS, groups)),
            dma((CHUNKS, groups)),
            dma((2,)),
            dma((2,)),
            dma((groups,)),
            dma((groups,)),
        ],
        compiler_params=pltpu.CompilerParams(
            collective_id=0, has_side_effects=True, vmem_limit_bytes=63 * 1024 * 1024
        ),
    )(
        tokens,
        targets,
        (loss_weights / seq)[:, None],
        segments.reshape(seq, 1),
        segments.reshape(1, seq),
        2.0 * probe_model.astype(F32) - 1.0,
        2.0 * probe_heads[0].astype(F32) - 1.0,
        norm_gain[None, :],
        cosine,
        sine,
        w_query,
        w_key,
        w_value,
        w_out,
    )
    mean_diag = jnp.stack([means[0, 0], means[0, HEAD_DIM // 2]])
    return (diag_query, diag_key, mean_diag)


def solution(mesh):
    placed = (
        P("dp", None),
        P("dp", None),
        P("dp"),
        P("dp", None),
        P("dp", None),
        P("dp", None, "mp"),
        P(),
        P(None, "mp"),
        P(None, "mp"),
        P(None, "mp"),
        P("mp", None),
    )
    return jax.shard_map(
        local,
        mesh=mesh,
        in_specs=placed,
        out_specs=(P("dp", "mp"), P("dp", "mp"), P()),
        check_vma=False,
    )
```
